32 devices in a mesh: groups: 2 (over x), rows: 4 (over y, core), cols: 4 (over z).
Axes of the slice: x: 2, y: 2, z: 4, core: 2. Of those that a mesh axis runs over, the one named last changes fastest.
Arguments:
- pair_state: float32 [768, 384, 128], P(('groups', 'rows'), 'cols'), parts along dimension 0, may hold values from -6 to 6
- token_mask: int32 [768], P('groups'), parts along dimension 0, may hold values 0 or 1
- norm_gain: float32 [2, 128], replicated, may hold values from 0.25 to 1.75
- norm_bias: float32 [2, 128], replicated, may hold values from -3 to 3
- proj_weight: float32 [2, 128, 512], replicated, may hold values from -0.5 to 0.5
- gate_weight: float32 [2, 128, 128], replicated, may hold values from -0.5 to 0.5
- out_gain: float32 [2, 128], replicated, may hold values from 0.25 to 1.75
- out_bias: float32 [2, 128], replicated, may hold values from -3 to 3
- out_weight: float32 [2, 128, 128], replicated, may hold values from -0.5 to 0.5
Outputs:
- pair_out: float32 [768, 384, 128], P(('groups', 'rows'), 'cols'), parts along dimension 0
The draws below stay inside these ranges and needn't reach their ends.
There are 2 independent parts, one for each index of `groups`. The reference program is written for one: setup_inputs(seed, part) draws one part's arguments, and reference() takes and returns one part's arrays. A program takes and returns all parts, laid end to end along the dimension named above; an argument that names none is the same for every part. Nothing has to cross between parts.
All inputs are finite; a program needn't handle non-finite values.
Results may differ from the reference program's by a relative error of at most 0.0001.
Values sent between devices are 32-bit elements; how exact they have to be, the bound alone decides.
A program may use at most 128 MiB of HBM per device.

```python
import jax
import jax.numpy as jnp
from jax import lax

C = 128
H = 128
N = 384


def plant(array, rng, least, high):
    shape = array.shape
    place = [jax.random.randint(jax.random.fold_in(rng, axis), (), 0, shape[axis]) for axis in range(len(shape))]
    array = array.at[tuple(place)].set(least)
    longest = shape.index(max(shape))
    place[longest] = (place[longest] + 1) % shape[longest]
    return array.at[tuple(place)].set(high)


def block_scale(stream_key, extent, pieces, smallest, top_value):
    def one(axis_at, shards_of):
        draws = jax.random.uniform(jax.random.fold_in(jax.random.fold_in(stream_key, 6), axis_at), (shards_of,), jnp.float32, smallest / len(pieces), top_value / len(pieces))
        return jnp.repeat(jnp.exp(draws), extent[axis_at] // shards_of).reshape((-1,) + (1,) * (len(extent) - axis_at - 1))

    level = one(*pieces[0])
    for cut in pieces[1:]:
        level = level * one(*cut)
    return level


def scatter_about(rng, shape, scale, limit, cuts=(), dtype=jnp.bfloat16):
    level = block_scale(rng, shape, cuts, -0.22, 0.18) if cuts else 1.0
    values = jax.random.normal(rng, shape, jnp.float32) * scale * level
    return jnp.minimum(jnp.maximum(values, -limit), limit).astype(dtype)


def setup_inputs(seed: int = 0, part: int = 0) -> dict:
    streams_of = jax.random.split(jax.random.key(seed), 10)
    part_keys = jax.random.split(jax.random.fold_in(streams_of[9], part), 10)
    return {
        "pair_state": scatter_about(part_keys[0], (N, N, C), 1.0, 6.0, ((0, 4), (1, 4)), jnp.float32),
        "token_mask": plant((jax.random.randint(part_keys[1], (N,), 0, 4) < 3).astype(jnp.int32), jax.random.fold_in(part_keys[1], 1), 0, 1),
        "norm_gain": jnp.clip(1.0 + 0.15 * jax.random.normal(streams_of[2], (2, C), jnp.float32), 0.25, 1.75),
        "norm_bias": scatter_about(streams_of[3], (2, C), 0.5, 3.0, (), jnp.float32),
        "proj_weight": scatter_about(streams_of[4], (2, C, 4 * H), C ** -0.5, 0.5, (), jnp.float32),
        "gate_weight": scatter_about(streams_of[5], (2, C, C), C ** -0.5, 0.5, (), jnp.float32),
        "out_gain": jnp.clip(1.0 + 0.15 * jax.random.normal(streams_of[6], (2, H), jnp.float32), 0.25, 1.75),
        "out_bias": scatter_about(streams_of[7], (2, H), 0.5, 3.0, (), jnp.float32),
        "out_weight": scatter_about(streams_of[8], (2, H, C), H ** -0.5, 0.5, (), jnp.float32),
    }


eps = 1e-05

def normalize(values, gain, shift):
    center = values - lax.optimization_barrier(jnp.mean(values, axis=-1, keepdims=True))
    spread = lax.optimization_barrier(jnp.mean(center * center, axis=-1, keepdims=True))
    return center * lax.rsqrt(spread + eps) * gain + shift

def update_once(state, pair_mask, segment, norm_gain, norm_bias, proj_weight, gate_weight, out_gain, out_bias, out_weight):
    width = proj_weight.shape[2] // 4
    normed = normalize(state, norm_gain[segment], norm_bias[segment])
    hidden = jnp.einsum('ijc,cf->ijf', normed, proj_weight[segment], precision=lax.Precision.HIGHEST)
    left_side = pair_mask[:, :, None] * jax.nn.sigmoid(hidden[:, :, :width]) * hidden[:, :, width:2 * width]
    right_side = pair_mask[:, :, None] * jax.nn.sigmoid(hidden[:, :, 2 * width:3 * width]) * hidden[:, :, 3 * width:]
    gating = jax.nn.sigmoid(jnp.einsum('ijc,cd->ijd', normed, gate_weight[segment], precision=lax.Precision.HIGHEST))
    if segment == 0:
        mixed = jnp.einsum('ikh,jkh->ijh', left_side, right_side, precision=lax.Precision.HIGHEST)
    else:
        mixed = jnp.einsum('kih,kjh->ijh', left_side, right_side, precision=lax.Precision.HIGHEST)
    result = jnp.einsum('ijh,hc->ijc', normalize(mixed, out_gain[segment], out_bias[segment]), out_weight[segment], precision=lax.Precision.HIGHEST)
    return state + gating * result

def reference(pair_state, token_mask, norm_gain, norm_bias, proj_weight, gate_weight, out_gain, out_bias, out_weight):
    maskf = token_mask.astype(jnp.float32)
    pair_mask = maskf[:, None] * maskf[None, :]
    state = pair_state
    for segment in range(2):
        state = update_once(state, pair_mask, segment, norm_gain, norm_bias, proj_weight, gate_weight, out_gain, out_bias, out_weight)
    return state
```

```python
import functools

import jax
import jax.numpy as jnp
from jax import lax
from jax.experimental.layout import Layout, with_layout_constraint
from jax.sharding import PartitionSpec as P

eps = 1e-05
precise = lax.Precision.HIGH


def normalize(values, gain, shift):
    center = values - jnp.mean(values, axis=-1, keepdims=True)
    spread = jnp.mean(center * center, axis=-1, keepdims=True)
    return center * lax.rsqrt(spread + eps) * gain + shift


def project(state, pair_mask, segment, norm_gain, norm_bias, proj_weight, gate_weight):
    width = proj_weight.shape[2] // 4
    normed = normalize(state, norm_gain[segment], norm_bias[segment])
    hidden = jnp.einsum(
        "ijc,cf->ijf", normed, proj_weight[segment], precision=precise
    )
    left_side = (
        pair_mask[:, :, None]
        * jax.nn.sigmoid(hidden[:, :, :width])
        * hidden[:, :, width : 2 * width]
    )
    right_side = (
        pair_mask[:, :, None]
        * jax.nn.sigmoid(hidden[:, :, 2 * width : 3 * width])
        * hidden[:, :, 3 * width :]
    )
    gating = jax.nn.sigmoid(
        jnp.einsum("ijc,cd->ijd", normed, gate_weight[segment], precision=precise)
    )
    return (left_side, right_side, gating)


def finish(state, mixed, gating, segment, out_gain, out_bias, out_weight):
    result = jnp.einsum(
        "ijh,hc->ijc",
        normalize(mixed, out_gain[segment], out_bias[segment]),
        out_weight[segment],
        precision=precise,
    )
    return state + gating * result


def plain_body(
    pair_state,
    token_mask,
    norm_gain,
    norm_bias,
    proj_weight,
    gate_weight,
    out_gain,
    out_bias,
    out_weight,
):
    row_count = pair_state.shape[0]
    col_count = pair_state.shape[1]
    row_start = lax.axis_index("rows") * row_count
    col_start = lax.axis_index("cols") * col_count
    maskf = token_mask.astype(jnp.float32)
    row_mask = lax.dynamic_slice_in_dim(maskf, row_start, row_count)
    col_mask = lax.dynamic_slice_in_dim(maskf, col_start, col_count)
    pair_mask = row_mask[:, None] * col_mask[None, :]
    left_side, right_side, gating = project(
        pair_state, pair_mask, 0, norm_gain, norm_bias, proj_weight, gate_weight
    )
    partial_out = jnp.einsum(
        "ikh,jkh->ijh",
        left_side,
        lax.all_gather(right_side, "rows", axis=0, tiled=True),
        precision=precise,
    )
    mixed = lax.psum_scatter(partial_out, "cols", scatter_dimension=1, tiled=True)
    updated = finish(pair_state, mixed, gating, 0, out_gain, out_bias, out_weight)
    left_next, right_next, gate_next = project(
        updated, pair_mask, 1, norm_gain, norm_bias, proj_weight, gate_weight
    )
    partial_in = jnp.einsum(
        "kih,kjh->ijh",
        lax.all_gather(left_next, "cols", axis=1, tiled=True),
        right_next,
        precision=precise,
    )
    mixed_next = lax.psum_scatter(partial_in, "rows", scatter_dimension=0, tiled=True)
    return finish(updated, mixed_next, gate_next, 1, out_gain, out_bias, out_weight)


def after(value, *earlier):
    return lax.optimization_barrier((value,) + earlier)[0]


def plain(value):
    return with_layout_constraint(value, Layout(major_to_minor=tuple(range(value.ndim))))


def pick(parts, index):
    return lax.dynamic_index_in_dim(parts, index, 0, keepdims=False)


def line_gather(block, axis, size, stride):
    lanes = range(stride)
    right, left = [], []
    going_right = going_left = block
    for step in range(size - 1):
        going_right = lax.ppermute(
            going_right, axis,
            [(c * stride + q, (c + 1) * stride + q) for c in range(step, size - 1) for q in lanes],
        )
        going_left = lax.ppermute(
            going_left, axis,
            [(c * stride + q, (c - 1) * stride + q) for c in range(1, size - step) for q in lanes],
        )
        right.append(going_right)
        left.append(going_left)
    return [block] + [right[t] + left[size - 2 - t] for t in range(size - 1)]


def line_scatter(chunk_of, here, axis, size, stride):
    lanes = range(stride)
    right = left = None
    marks = []
    for step in range(size - 1):
        ahead = size - 1 - step
        send_right = chunk_of(jnp.minimum(here + ahead, size - 1))
        send_left = chunk_of(jnp.maximum(here - ahead, 0))
        if step:
            send_right = send_right + right
            send_left = send_left + left
        right = lax.ppermute(
            send_right, axis,
            [(c * stride + q, (c + 1) * stride + q) for c in range(step + 1) for q in lanes],
        )
        left = lax.ppermute(
            send_left, axis,
            [(c * stride + q, (c - 1) * stride + q) for c in range(size - 1 - step, size) for q in lanes],
        )
        marks.append(right)
    own = chunk_of(here)
    return (own if right is None else own + right + left), marks


def gated(normed, mask, weight, first, width):
    hidden = jnp.einsum("ijc,cf->ijf", normed, weight[:, first : first + 2 * width], precision=precise)
    return mask[:, :, None] * jax.nn.sigmoid(hidden[:, :, :width]) * hidden[:, :, width:]


def gate_of(normed, weight):
    return jax.nn.sigmoid(jnp.einsum("ijc,cd->ijd", normed, weight, precision=precise))


def body(rows, cols, pieces, pair_state, token_mask, norm_gain, norm_bias, proj_weight,
         gate_weight, out_gain, out_bias, out_weight):
    width = proj_weight.shape[2] // 4
    extent = pair_state.shape[0]
    small = extent // pieces
    row_at, col_at = lax.axis_index("rows"), lax.axis_index("cols")
    chips = rows // 2
    chip, core = row_at // 2, row_at % 2
    swap = [(r, r ^ 1) for r in range(rows)]
    maskf = token_mask.astype(jnp.float32)
    pair_mask = (
        lax.dynamic_slice_in_dim(maskf, row_at * extent, extent)[:, None]
        * lax.dynamic_slice_in_dim(maskf, col_at * extent, extent)[None, :]
    )
    spans = [slice(p * small, (p + 1) * small) for p in range(pieces)]

    normed = normalize(pair_state, norm_gain[0], norm_bias[0])
    gathered = []
    for span in spans:
        right_side = gated(normed[span], pair_mask[span], proj_weight[0], 2 * width, width)
        near = jnp.stack(line_gather(right_side, "rows", chips, 2))
        far = lax.ppermute(near, "rows", swap)
        gathered.append(jnp.stack([near, far], axis=1).reshape((rows,) + right_side.shape))
    left_side = gated(normed, pair_mask, proj_weight[0], 0, width)

    updated, right_next, gate_next, left_all, marks = [], [], [], [], []
    for p, span in enumerate(spans):
        block = after(gathered[p], marks[p - 2][0]) if p >= 2 else gathered[p]
        partial = plain(jnp.einsum("ikh,djkh->dijh", left_side, block, precision=precise))

        def chunk_of(d, partial=partial):
            return pick(partial, ((chip - d // 2 + chips) % chips) * 2 + (d % 2 + core) % 2)

        mixed, mark = line_scatter(chunk_of, col_at, "cols", cols, 1)
        marks.append(mark)
        state = finish(
            pair_state[:, span], mixed, gate_of(normed[:, span], gate_weight[0]),
            0, out_gain, out_bias, out_weight,
        )
        again = normalize(state, norm_gain[1], norm_bias[1])
        left_next = gated(again, pair_mask[:, span], proj_weight[1], 0, width)
        left_all.append(line_gather(left_next, "cols", cols, 1))
        right_next.append(gated(again, pair_mask[:, span], proj_weight[1], 2 * width, width))
        gate_next.append(gate_of(again, gate_weight[1]))
        updated.append(state)

    right_whole = jnp.concatenate(right_next, axis=1)
    gate_whole = jnp.concatenate(gate_next, axis=1)
    state_whole = jnp.concatenate(updated, axis=1)
    results, marks = [], []
    for p, span in enumerate(spans):
        block = jnp.stack(left_all[p])
        block = after(block, marks[p - 2][0]) if p >= 2 else block
        partial = jnp.einsum("dkih,kjh->dijh", block, right_whole, precision=precise)

        def block_of(b, partial=partial):
            return pick(partial, (col_at - b + cols) % cols)

        kept = jnp.stack([block_of(2 * y + core) for y in range(chips)])
        sent = jnp.stack([block_of(2 * y + 1 - core) for y in range(chips)])
        both = kept + lax.ppermute(sent, "rows", swap)
        mixed, mark = line_scatter(lambda y, both=both: pick(both, y), chip, "rows", chips, 2)
        marks.append(mark)
        results.append(
            finish(state_whole[span], mixed, gate_whole[span], 1, out_gain, out_bias, out_weight)
        )
    return jnp.concatenate(results, axis=0)


def solution(mesh):
    placed = (P(("groups", "rows"), "cols", None), P("groups"), P(), P(), P(), P(), P(), P(), P())
    rows, cols = mesh.shape["rows"], mesh.shape["cols"]
    if rows == cols and rows % 2 == 0:
        run = functools.partial(body, rows, cols, 4)
    else:
        run = plain_body
    return jax.shard_map(
        run,
        mesh=mesh,
        in_specs=placed,
        out_specs=P(("groups", "rows"), "cols", None),
        check_vma=False,
    )
```
